32 devices in a mesh: dp: 2 (over y), expert: 16 (over z, x, core).
Axes of the slice: x: 2, y: 2, z: 4, core: 2. Of those that a mesh axis runs over, the one named last changes fastest.
Arguments:
- tokens: bfloat16 [512, 4096], P(('dp', 'expert')), may hold values from -6 to 6
- routing: int32 [512, 2], P(('dp', 'expert')), may hold values from 0 to 7, as said below
- hidden_grad: bfloat16 [2048, 4096], P(('dp', 'expert')), may hold values from -3 to 3
- gate_weight: bfloat16 [4096, 65536], P(None, 'expert'), may hold values from -0.09375 to 0.09375
- up_weight: bfloat16 [4096, 65536], P(None, 'expert'), may hold values from -0.09375 to 0.09375
Outputs:
- token_grad: bfloat16 [512, 4096], P(('dp', 'expert'))
- gate_weight_grad: bfloat16 [4096, 65536], P('dp', 'expert')
- up_weight_grad: bfloat16 [4096, 65536], P('dp', 'expert')
The draws below stay inside these ranges and needn't reach their ends.
Inputs may be any that keep to these rules, and one draw needn't show every extreme that they name: `routing`: the 2 entries of a token differ, and no device names one expert in more than 4 of its tokens.
All inputs are finite; a program needn't handle non-finite values.
Results may differ from the reference program's by a relative error of at most 0.0085.
Values may be sent and summed in bfloat16 or wider, within the bound.
A program may use at most 256 MiB of HBM per device.

```python
import jax
import jax.numpy as jnp
from jax import lax

D = 4096
EXPERTS = 8
TOP = 2
FF = 8192
CAP = 4
TOK = 16
FFD = 4096
ROWS = 64
TOKENS = 512
N_DP = 2
N_EXPERT = 16
DEVICES = 32


def draw_routing(key, part):
    hot_expert = jax.random.randint(jax.random.fold_in(key, 11), (), 0, EXPERTS)
    block_keys = jax.random.split(jax.random.fold_in(key, 12), TOKENS // TOK)

    def one_block(block_key):
        key_order, key_cycle, key_offset, key_flip = jax.random.split(block_key, 4)
        order = jax.random.permutation(key_order, TOK)
        token_rank = jnp.argsort(order, stable=True).astype(jnp.int32)
        cycle = jax.random.permutation(key_cycle, EXPERTS - 1).astype(jnp.int32)
        offset = jax.random.randint(key_offset, (), 0, EXPERTS - 1)
        flipped = jax.random.randint(key_flip, (TOK,), 0, 2)
        first_index = token_rank + jnp.maximum(token_rank - CAP, 0)

        def other_expert(index):
            return (hot_expert + 1 + cycle[(index + offset) % (EXPERTS - 1)]) % EXPERTS
        first_other = other_expert(first_index)
        second_other = other_expert(first_index + 1)
        is_hot = token_rank < CAP
        column_a = jnp.where(is_hot, jnp.where(flipped == 1, hot_expert, first_other), first_other)
        column_b = jnp.where(is_hot, jnp.where(flipped == 1, first_other, hot_expert), second_other)
        return jnp.stack([column_a, column_b], axis=1)
    return jax.vmap(one_block)(block_keys).reshape(TOKENS, TOP).astype(jnp.int32)


def level_of(own_key, extent, cuts, least, top_value):
    gain = 1.0
    for axis_at, shards_of in cuts:
        steps = jax.random.uniform(jax.random.fold_in(jax.random.fold_in(own_key, 6), axis_at), (shards_of,), jnp.float32, least / len(cuts), top_value / len(cuts))
        gain = gain * jnp.repeat(jnp.exp(steps), extent[axis_at] // shards_of).reshape((-1,) + (1,) * (len(extent) - 1 - axis_at))
    return gain


def normal_values(rng, dims, deviation, limit, pieces=(), held_as=jnp.bfloat16):
    values = jax.random.normal(rng, dims, jnp.float32) * deviation
    if len(pieces) > 0:
        values = level_of(rng, dims, pieces, -0.22, 0.18) * values
    return jnp.clip(values, min=-limit, max=limit).astype(held_as)


def setup_inputs(seed: int = 0) -> dict:
    arg_keys = jax.random.split(jax.random.key(seed), 6)
    tokens = normal_values(arg_keys[0], (TOKENS, D), 1.0, 6.0, ((0, 32),))
    routing = draw_routing(jax.random.fold_in(arg_keys[5], 71), 0)
    hidden_grad = normal_values(arg_keys[2], (DEVICES * ROWS, FFD), 0.5, 3.0, ((0, 32),))
    gate_weight = normal_values(arg_keys[3], (D, EXPERTS * FF), D ** -0.5, 0.09375, ((1, 16),))
    up_weight = normal_values(arg_keys[4], (D, EXPERTS * FF), D ** -0.5, 0.09375, ((1, 16),))
    return dict(tokens=tokens, routing=routing, hidden_grad=hidden_grad, gate_weight=gate_weight, up_weight=up_weight)


def slot_tables(routing_dev):
    flat_experts = routing_dev.reshape(-1)
    onehot = (flat_experts[:, None] == jnp.arange(EXPERTS, dtype=jnp.int32)[None, :]).astype(jnp.int32)
    before = jnp.cumsum(onehot, axis=0) - onehot
    slot_index = jnp.sum(before * onehot, axis=1)
    target = flat_experts * CAP + slot_index
    placed = target[:, None] == jnp.arange(EXPERTS * CAP, dtype=jnp.int32)[None, :]
    return placed.astype(jnp.float32)


def reference(tokens, routing, hidden_grad, gate_weight, up_weight):
    shards = N_EXPERT // EXPERTS
    ffd_cols = FF // shards
    row_count = N_EXPERT * CAP
    token_blocks = tokens.reshape(N_DP, N_EXPERT, TOK, D)
    route_blocks = routing.reshape(N_DP, N_EXPERT, TOK, TOP)
    placed = jax.vmap(jax.vmap(slot_tables))(route_blocks)
    doubled = jnp.repeat(token_blocks, TOP, axis=2).astype(jnp.float32)
    outgoing = jnp.einsum('rsae,rsad->rsed', placed, doubled, precision=lax.Precision.HIGHEST)
    outgoing = outgoing.astype(jnp.bfloat16).reshape(N_DP, N_EXPERT, EXPERTS, CAP, D)
    expert_inputs = outgoing.transpose(2, 0, 1, 3, 4).reshape(EXPERTS, N_DP, row_count, D)
    grad_blocks = hidden_grad.reshape(N_DP, EXPERTS, shards, row_count, ffd_cols).transpose(1, 0, 2, 3, 4)
    gate_blocks = gate_weight.reshape(D, EXPERTS, FF).transpose(1, 0, 2)
    up_blocks = up_weight.reshape(D, EXPERTS, FF).transpose(1, 0, 2)

    def one_expert(inputs):
        expert_x, expert_h, w_gate, w_up = inputs
        gate_total = jnp.zeros((D, FF), jnp.float32)
        up_total = jnp.zeros((D, FF), jnp.float32)
        sums = []
        for replica in range(N_DP):
            expert_rows = expert_x[replica]
            gate_pre = jnp.dot(expert_rows, w_gate, preferred_element_type=jnp.float32)
            up_pre = jnp.dot(expert_rows, w_up, preferred_element_type=jnp.float32)
            grad_h = expert_h[replica].transpose(1, 0, 2).reshape(row_count, FF).astype(jnp.float32)
            sigmoid_gate = jax.nn.sigmoid(gate_pre)
            gate_grad = (grad_h * up_pre * sigmoid_gate * (1.0 + gate_pre * (1.0 - sigmoid_gate))).astype(jnp.bfloat16)
            up_grad = (grad_h * gate_pre * sigmoid_gate).astype(jnp.bfloat16)
            first_part = jnp.einsum('rsf,dsf->srd', gate_grad.reshape(row_count, shards, ffd_cols).astype(jnp.float32),
                                    w_gate.reshape(D, shards, ffd_cols).astype(jnp.float32))
            second_part = jnp.einsum('rsf,dsf->srd', up_grad.reshape(row_count, shards, ffd_cols).astype(jnp.float32),
                                     w_up.reshape(D, shards, ffd_cols).astype(jnp.float32))
            partial_value = (first_part + second_part).astype(jnp.bfloat16).astype(jnp.float32)
            sums.append(jnp.sum(partial_value, axis=0))
            gate_term = jnp.dot(expert_rows.T, gate_grad, preferred_element_type=jnp.float32)
            up_term = jnp.dot(expert_rows.T, up_grad, preferred_element_type=jnp.float32)
            gate_total = gate_total + gate_term.astype(jnp.bfloat16).astype(jnp.float32)
            up_total = up_total + up_term.astype(jnp.bfloat16).astype(jnp.float32)
        return jnp.stack(sums), gate_total.astype(jnp.bfloat16), up_total.astype(jnp.bfloat16)

    partial_sums, gate_grads, up_grads = lax.map(one_expert, (expert_inputs, grad_blocks, gate_blocks, up_blocks))
    back = partial_sums.reshape(EXPERTS, N_DP, N_EXPERT, CAP, D).transpose(1, 2, 0, 3, 4)
    back = back.reshape(N_DP, N_EXPERT, EXPERTS * CAP, D)
    gathered = jnp.einsum('rsae,rsed->rsad', placed, back, precision=lax.Precision.HIGHEST)
    token_grad = jnp.sum(gathered.reshape(N_DP, N_EXPERT, TOK, TOP, D), axis=3).astype(jnp.bfloat16)
    token_grad = token_grad.reshape(TOKENS, D)
    gate_weight_grad = gate_grads.transpose(1, 0, 2).reshape(D, EXPERTS * FF)
    up_weight_grad = up_grads.transpose(1, 0, 2).reshape(D, EXPERTS * FF)
    return token_grad, gate_weight_grad, up_weight_grad
```

```python
import functools

import jax
import jax.numpy as jnp
from jax import lax
from jax.experimental import pallas as pl
from jax.experimental.pallas import tpu as pltpu
from jax.sharding import PartitionSpec as P


EXPERTS = 8
CAP = 4
MIB = 1024 * 1024

BLOCK = 512
SLOTS = 6
TILE = 256
WEIGHT_BLOCK = 256
MESH = pl.DeviceIdType.MESH
TRANSPOSED = (((1,), (1,)), ((), ()))
LEADING = (((0,), (0,)), ((), ()))


def placement(routing, columns, expert_of, part_of, slot_of):
    count = routing.shape[0]
    column = lax.broadcasted_iota(jnp.int32, (count, columns), 1)
    expert, part, slot = expert_of(column), part_of(column), slot_of(column)
    first = jnp.where(routing[:, 0:1] == expert, 1.0, 0.0)
    second = jnp.where(routing[:, 1:2] == expert, 1.0, 0.0)
    earlier = jnp.where(
        lax.broadcasted_iota(jnp.int32, (count, count), 0)
        > lax.broadcasted_iota(jnp.int32, (count, count), 1),
        1.0,
        0.0,
    )
    before = jnp.dot(earlier, first + second, preferred_element_type=jnp.float32)
    slot = slot.astype(jnp.float32)
    placed = jnp.where(before == slot, first, 0.0) + jnp.where(before + first == slot, second, 0.0)
    return [jnp.where(part == h, placed, 0.0).astype(jnp.bfloat16) for h in range(2)]


def row_picker(rows, half):
    at = lax.broadcasted_iota(jnp.int32, (rows, 2 * rows), 0)
    column = lax.broadcasted_iota(jnp.int32, (rows, 2 * rows), 1)
    wanted = (at // CAP) * (2 * CAP) + at % CAP + half * CAP
    return jnp.where(column == wanted, 1.0, 0.0).astype(jnp.bfloat16)


def row_spreader(rows, half):
    column = lax.broadcasted_iota(jnp.int32, (2 * rows, rows), 1)
    at = lax.broadcasted_iota(jnp.int32, (2 * rows, rows), 0)
    wanted = (column // CAP) * (2 * CAP) + column % CAP + half * CAP
    return jnp.where(at == wanted, 1.0, 0.0).astype(jnp.bfloat16)


def hidden_kernel(
    dims,
    routing_ref, tokens_ref, hidden_hbm, gate_hbm, up_hbm,
    grads_hbm, half_ref, part_ref,
    out, parts, rows, hid, wts, total, grads,
    wts_sem, own_sem, grads_sem,
    hid_send, hid_recv, row_send, row_recv, side_send, side_recv,
    far_send, far_recv, last_send, last_recv,
):
    n_dp, n_expert, block, slots = dims
    replica, index = lax.axis_index("dp"), lax.axis_index("expert")
    shards = n_expert // EXPERTS
    peers = n_expert // 2
    chip, core = index // 2, index % 2
    sibling = chip * 2 + 1 - core
    other = 1 - replica
    count, width = rows.shape
    half = width // 2
    mine = width // n_dp
    steps = gate_hbm.shape[1] // block

    def weight_copies(step, slot):
        columns = pl.ds(pl.multiple_of(step * block, block), block)
        return (
            pltpu.make_async_copy(gate_hbm.at[:, columns], wts.at[slot, 0], wts_sem.at[slot, 0]),
            pltpu.make_async_copy(up_hbm.at[:, columns], wts.at[slot, 1], wts_sem.at[slot, 1]),
        )

    def own_copy(step):
        columns = pl.ds(pl.multiple_of(step * block, block), block)
        return pltpu.make_async_copy(hidden_hbm.at[:, columns], hid.at[step, replica], own_sem.at[step])

    def grads_copy(step):
        columns = pl.ds(pl.multiple_of(step * block, block), block)
        return pltpu.make_async_copy(grads.at[step], grads_hbm.at[:, :, columns], grads_sem.at[step])

    def peer(apart):
        return lax.rem(chip + apart + peers, peers) * 2 + core

    def place(replica_at, device):
        return replica_at * n_expert + device

    def hid_copy(step):
        return pltpu.make_async_remote_copy(
            hid.at[step, replica], hid.at[step, replica], hid_send.at[step], hid_recv.at[step],
            device_id=(other, index), device_id_type=MESH,
        )

    def hid_arrival(step):
        return pltpu.make_async_remote_copy(
            hid.at[step, other], hid.at[step, other], hid_send.at[step], hid_recv.at[step],
            device_id=(other, index), device_id_type=MESH,
        )

    def row_copy(apart):
        return pltpu.make_async_remote_copy(
            out.at[peer(apart) // shards], parts.at[place(replica, index)],
            row_send.at[apart], row_recv.at[apart],
            device_id=(replica, peer(apart)), device_id_type=MESH,
        )

    def moved(source, at, send, recv, apart, to):
        return pltpu.make_async_remote_copy(
            source, parts.at[at], send.at[apart], recv.at[apart], device_id=to, device_id_type=MESH
        )

    for step in range(steps):
        own_copy(step).start()
    for step in range(slots):
        for copy in weight_copies(step, step):
            copy.start()

    barrier = pltpu.get_barrier_semaphore()

    def greet(apart, carry):
        pl.semaphore_signal(barrier, inc=1, device_id=(replica, peer(apart)), device_id_type=MESH)
        return carry

    lax.fori_loop(1, peers, greet, 0)
    pl.semaphore_signal(barrier, inc=1, device_id=(replica, sibling), device_id_type=MESH)
    pl.semaphore_signal(barrier, inc=1, device_id=(other, index), device_id_type=MESH)

    picks = placement(
        routing_ref[...], EXPERTS * 2 * CAP,
        lambda j: j // (2 * CAP), lambda j: (j // CAP) % 2, lambda j: j % CAP,
    )
    sent = lax.dot_general(
        picks[0], tokens_ref[:, :half], LEADING, preferred_element_type=jnp.float32
    ) + lax.dot_general(picks[1], tokens_ref[:, half:], LEADING, preferred_element_type=jnp.float32)
    out[...] = sent.astype(jnp.bfloat16).reshape(out.shape)
    parts[place(replica, index)] = out[index // shards]
    total[...] = jnp.zeros_like(total)

    pl.semaphore_wait(barrier, peers + 1)

    def dispatch(apart, carry):
        row_copy(apart).start()
        return carry

    lax.fori_loop(1, peers, dispatch, 0)
    own_block = out.at[index // shards]
    own_at = place(replica, index)
    moved(own_block, own_at, side_send, side_recv, 0, (replica, sibling)).start()
    moved(own_block, own_at, far_send, far_recv, 0, (other, index)).start()
    early = min(2, steps)
    for step in range(early):
        own_copy(step).wait()
        hid_copy(step).start()

    def pass_on(apart, carry):
        at = place(replica, peer(-apart))
        moved(parts.at[at], at, row_send, row_recv, apart, (replica, sibling)).wait_recv()
        moved(parts.at[at], at, side_send, side_recv, apart, (replica, sibling)).start()
        moved(parts.at[at], at, far_send, far_recv, apart, (other, index)).start()
        return carry

    lax.fori_loop(1, peers, pass_on, 0)
    for step in range(early, steps):
        own_copy(step).wait()
        hid_copy(step).start()

    def share(apart, carry):
        at = place(other, peer(-apart))
        moved(parts.at[at], at, far_send, far_recv, apart, (other, index)).wait_recv()
        moved(parts.at[at], at, last_send, last_recv, apart, (replica, sibling)).start()
        return carry

    lax.fori_loop(0, peers, share, 0)

    def settle(apart, carry):
        their = lax.rem(chip - apart + peers, peers) * 2 + 1 - core
        at = place(replica, their)
        moved(parts.at[at], at, side_send, side_recv, apart, (replica, sibling)).wait_recv()
        at = place(other, their)
        moved(parts.at[at], at, last_send, last_recv, apart, (replica, sibling)).wait_recv()
        return carry

    lax.fori_loop(0, peers, settle, 0)

    group = min(count, 128)
    for h in range(2):
        pick = row_picker(group, h)
        for at in range(0, count, group):
            got = parts[pl.ds(at // CAP, group // CAP)].reshape(2 * group, half)
            rows[at : at + group, h * half : (h + 1) * half] = jnp.dot(
                pick, got, preferred_element_type=jnp.float32
            ).astype(jnp.bfloat16)

    def forward(slot, at):
        columns = pl.ds(at, TILE)
        gate_pre = jnp.dot(rows[...], wts[slot, 0, :, columns], preferred_element_type=jnp.float32)
        up_pre = jnp.dot(rows[...], wts[slot, 1, :, columns], preferred_element_type=jnp.float32)
        return gate_pre, up_pre

    def gradients(step, at, gate_pre, up_pre):
        grad_h = hid[step, :, :, at : at + TILE].reshape(count, TILE).astype(jnp.float32)
        sig = jax.nn.sigmoid(gate_pre)
        grads[step, 0, :, at : at + TILE] = (
            grad_h * up_pre * sig * (1.0 + gate_pre * (1.0 - sig))
        ).astype(jnp.bfloat16)
        grads[step, 1, :, at : at + TILE] = (grad_h * gate_pre * sig).astype(jnp.bfloat16)

    first_row = pl.multiple_of(replica * mine, mine)

    def backward(step, slot, at):
        features = pl.ds(first_row + at, TILE)
        total[:, at : at + TILE] += lax.dot_general(
            grads[step, 0], wts[slot, 0, features, :], TRANSPOSED, preferred_element_type=jnp.float32
        ) + lax.dot_general(
            grads[step, 1], wts[slot, 1, features, :], TRANSPOSED, preferred_element_type=jnp.float32
        )

    def ready(step, slot):
        for copy in weight_copies(step, slot):
            copy.wait()
        hid_arrival(step).wait_recv()

    ready(0, 0)
    for at in range(0, block, TILE):
        gradients(0, at, *forward(0, at))
    grads_copy(0).start()
    tiles = block // TILE
    share_of = mine // tiles

    def advance(step, carry):
        slot, before = lax.rem(step, slots), lax.rem(step - 1, slots)
        ready(step, slot)
        for tile in range(tiles):
            pre = forward(slot, tile * TILE)
            for at in range(tile * share_of, (tile + 1) * share_of, TILE):
                backward(step - 1, before, at)
            gradients(step, tile * TILE, *pre)
        grads_copy(step).start()

        @pl.when(step - 1 + slots < steps)
        def _():
            for copy in weight_copies(step - 1 + slots, before):
                copy.start()

        return carry

    lax.fori_loop(1, steps, advance, 0)
    for at in range(0, mine, TILE):
        backward(steps - 1, (steps - 1) % slots, at)

    half_ref[...] = rows[:, pl.ds(first_row, mine)]
    quarter = mine // 2
    for at in range(0, count, group):
        kept = total[at : at + group].astype(jnp.bfloat16)
        spread = jnp.dot(
            row_spreader(group, 0), kept[:, :quarter], preferred_element_type=jnp.float32
        ) + jnp.dot(row_spreader(group, 1), kept[:, quarter:], preferred_element_type=jnp.float32)
        part_ref[pl.ds(at // CAP, group // CAP)] = spread.astype(jnp.bfloat16).reshape(
            group // CAP, 2 * CAP, quarter
        )

    for step in range(steps):
        grads_copy(step).wait()
        hid_copy(step).wait_send()

    def finish(apart, carry):
        row_copy(apart).wait_send()
        return carry

    lax.fori_loop(1, peers, finish, 0)

    def finish_moved(apart, carry):
        at = place(replica, peer(-apart))
        moved(parts.at[at], at, side_send, side_recv, apart, (replica, sibling)).wait_send()
        moved(parts.at[at], at, far_send, far_recv, apart, (other, index)).wait_send()
        moved(parts.at[at], at, last_send, last_recv, apart, (replica, sibling)).wait_send()
        return carry

    lax.fori_loop(0, peers, finish_moved, 0)


def hidden_pass(routing, tokens, hidden, gate_weight, up_weight):
    n_dp, n_expert = lax.axis_size("dp"), lax.axis_size("expert")
    width = tokens.shape[1]
    span = gate_weight.shape[1]
    count = n_dp * hidden.shape[0]
    block = min(BLOCK, span)
    steps = span // block
    slots = min(SLOTS, steps)
    peers = n_expert // 2
    mine = width // n_dp
    vmem = pl.BlockSpec(memory_space=pltpu.VMEM)
    anywhere = pl.BlockSpec(memory_space=pl.ANY)
    blocks = n_dp * n_expert
    dma = pltpu.SemaphoreType.DMA
    return pl.pallas_call(
        functools.partial(hidden_kernel, (n_dp, n_expert, block, slots)),
        in_specs=[vmem, vmem, anywhere, anywhere, anywhere],
        out_specs=[anywhere, vmem, vmem],
        out_shape=[
            jax.ShapeDtypeStruct((2, count, span), jnp.bfloat16),
            jax.ShapeDtypeStruct((count, mine), jnp.bfloat16),
            jax.ShapeDtypeStruct((blocks, 2 * CAP, mine // 2), jnp.bfloat16),
        ],
        scratch_shapes=[
            pltpu.VMEM((EXPERTS, 2 * CAP, width // 2), jnp.bfloat16),
            pltpu.VMEM((blocks, 2 * CAP, width // 2), jnp.bfloat16),
            pltpu.VMEM((count, width), jnp.bfloat16),
            pltpu.VMEM((steps, n_dp, hidden.shape[0], block), jnp.bfloat16),
            pltpu.VMEM((slots, 2, width, block), jnp.bfloat16),
            pltpu.VMEM((count, mine), jnp.float32),
            pltpu.VMEM((steps, 2, count, block), jnp.bfloat16),
            dma((slots, 2)), dma((steps,)), dma((steps,)),
            dma((steps,)), dma((steps,)),
            dma((peers,)), dma((peers,)), dma((peers,)), dma((peers,)),
            dma((peers,)), dma((peers,)), dma((peers,)), dma((peers,)),
        ],
        cost_estimate=pl.CostEstimate(
            flops=6 * count * width * span,
            bytes_accessed=4 * width * span,
            transcendentals=count * span,
        ),
        compiler_params=pltpu.CompilerParams(
            collective_id=0, has_side_effects=True, vmem_limit_bytes=62 * MIB
        ),
    )(routing, tokens, hidden, gate_weight, up_weight)


def weight_kernel(half_ref, grads_ref, gate_ref, up_ref, turned_ref):
    @pl.when(pl.program_id(0) == 0)
    def _():
        turned_ref[...] = half_ref[...].T

    for at, out_ref in ((0, gate_ref), (1, up_ref)):
        out_ref[...] = jnp.dot(
            turned_ref[...], grads_ref[at], preferred_element_type=jnp.float32
        ).astype(out_ref.dtype)


def weight_pass(half, grads):
    count, mine = half.shape
    span = grads.shape[2]
    block = min(WEIGHT_BLOCK, span)
    result = jax.ShapeDtypeStruct((mine, span), jnp.bfloat16)
    out = pl.BlockSpec((mine, block), lambda j: (0, j))
    return pl.pallas_call(
        weight_kernel,
        grid=(span // block,),
        in_specs=[
            pl.BlockSpec((count, mine), lambda j: (0, 0)),
            pl.BlockSpec((2, count, block), lambda j: (0, 0, j)),
        ],
        out_specs=[out, out],
        out_shape=[result, result],
        scratch_shapes=[pltpu.VMEM((mine, count), jnp.bfloat16)],
        cost_estimate=pl.CostEstimate(
            flops=4 * count * mine * span, bytes_accessed=4 * mine * span, transcendentals=0
        ),
        compiler_params=pltpu.CompilerParams(
            dimension_semantics=("arbitrary",), vmem_limit_bytes=40 * MIB
        ),
    )(half, grads)


def return_kernel(shards, n_dp, routing_ref, back_ref, out_ref):
    blocks, deep, quarter = back_ref.shape
    sources = blocks // n_dp
    picks = placement(
        routing_ref[...], sources * deep,
        lambda j: j // (deep * shards), lambda j: (j // CAP) % 2, lambda j: j % CAP,
    )
    for replica in range(n_dp):
        got = back_ref[pl.ds(replica * sources, sources)].reshape(sources * deep, quarter)
        for h in range(2):
            at = (2 * replica + h) * quarter
            out_ref[:, at : at + quarter] = jnp.dot(
                picks[h], got, preferred_element_type=jnp.float32
            ).astype(out_ref.dtype)


def return_pass(routing, back, width):
    n_dp = lax.axis_size("dp")
    shards = lax.axis_size("expert") // EXPERTS
    vmem = pl.BlockSpec(memory_space=pltpu.VMEM)
    return pl.pallas_call(
        functools.partial(return_kernel, shards, n_dp),
        in_specs=[vmem, vmem],
        out_specs=vmem,
        out_shape=jax.ShapeDtypeStruct((routing.shape[0], width), jnp.bfloat16),
    )(routing, back)


def per_device(tokens, routing, hidden_grad, gate_weight, up_weight):
    grads, half, part = hidden_pass(routing, tokens, hidden_grad, gate_weight, up_weight)
    back = lax.all_to_all(part, ("dp", "expert"), split_axis=0, concat_axis=0, tiled=True)
    gate_weight_grad, up_weight_grad = weight_pass(half, grads)
    token_grad = return_pass(routing, back, tokens.shape[1])
    return token_grad, gate_weight_grad, up_weight_grad


def solution(mesh):
    in_specs = (
        P(("dp", "expert"), None),
        P(("dp", "expert"), None),
        P(("dp", "expert"), None),
        P(None, "expert"),
        P(None, "expert"),
    )
    out_specs = (P(("dp", "expert"), None), P("dp", "expert"), P("dp", "expert"))
    return jax.shard_map(
        per_device, mesh=mesh, in_specs=in_specs, out_specs=out_specs, check_vma=False
    )
```

```python
import functools

import jax
import jax.numpy as jnp
from jax import lax
from jax.experimental import pallas as pl
from jax.experimental.pallas import tpu as pltpu
from jax.sharding import PartitionSpec as P


EXPERTS = 8
CAP = 4
CAP_BITS = CAP.bit_length() - 1
MIB = 1024 * 1024
KERNEL_MIB = 63

TILE = 256
WIDE = 512
PIECES = 4
BANDS = 4
EARLY_BANDS = 1
ROW_BLOCK = 256
MESH = pl.DeviceIdType.MESH
TRANSPOSED = (((1,), (1,)), ((), ()))
LEADING = (((0,), (0,)), ((), ()))


def placement(routing, rows, expert_bits):
    count = routing.shape[1]
    row = lax.broadcasted_iota(jnp.int32, (rows, count), 0)
    expert, part = row >> expert_bits, (row >> CAP_BITS) & 1
    slot = (row & (CAP - 1)).astype(jnp.float32)
    first = jnp.where(routing[0:1] == expert, 1.0, 0.0)
    second = jnp.where(routing[1:2] == expert, 1.0, 0.0)
    earlier = jnp.where(
        lax.broadcasted_iota(jnp.int32, (count, count), 0)
        < lax.broadcasted_iota(jnp.int32, (count, count), 1),
        1.0,
        0.0,
    )
    before = jnp.dot(first + second, earlier, preferred_element_type=jnp.float32)
    placed = jnp.where(before == slot, first, 0.0) + jnp.where(before + first == slot, second, 0.0)
    return [jnp.where(part == h, placed, 0.0).astype(jnp.bfloat16) for h in range(2)]


def row_picker(rows, half):
    at = lax.broadcasted_iota(jnp.int32, (rows, 2 * rows), 0)
    column = lax.broadcasted_iota(jnp.int32, (rows, 2 * rows), 1)
    wanted = ((at >> CAP_BITS) << (CAP_BITS + 1)) + (at & (CAP - 1)) + half * CAP
    return jnp.where(column == wanted, 1.0, 0.0).astype(jnp.bfloat16)


def row_spreader(rows, half):
    column = lax.broadcasted_iota(jnp.int32, (2 * rows, rows), 1)
    at = lax.broadcasted_iota(jnp.int32, (2 * rows, rows), 0)
    wanted = ((column >> CAP_BITS) << (CAP_BITS + 1)) + (column & (CAP - 1)) + half * CAP
    return jnp.where(at == wanted, 1.0, 0.0).astype(jnp.bfloat16)


def hidden_kernel(
    dims,
    routing_hbm, tokens_hbm, hidden_hbm, gate_hbm, up_hbm,
    grads_hbm, turned_hbm, part_ref,
    routing_ref, tokens_ref, grads_ref, turned_ref, out, parts, rows, hid, near, ring, pre, kept,
    near_sem, ring_sem, own_sem, grads_sem, turned_sem, routing_sem, tokens_sem,
    hid_send, hid_recv, row_send, row_recv, side_send, side_recv,
    far_send, far_recv, last_send, last_recv,
):
    _, n_expert = dims
    replica, index = lax.axis_index("dp"), lax.axis_index("expert")
    shards = n_expert // EXPERTS
    peers = n_expert // 2
    chip, core = index // 2, index % 2
    sibling = chip * 2 + 1 - core
    other = 1 - replica
    _, count, mine = rows.shape
    half = parts.shape[3]
    span = gate_hbm.shape[1]
    piece = mine // PIECES
    tile = min(TILE, span)
    weights = (gate_hbm, up_hbm)

    def near_copy(at, which):
        source = pl.ds(pl.multiple_of(replica * mine + at * piece, piece), piece)
        return pltpu.make_async_copy(
            weights[which].at[source], near.at[which, pl.ds(at * piece, piece)], near_sem.at[at, which]
        )

    def ring_copy(at, which):
        source = pl.ds(pl.multiple_of(other * mine + at * piece, piece), piece)
        return pltpu.make_async_copy(
            weights[which].at[source], ring.at[at % 2, which], ring_sem.at[at, which]
        )

    own_copy = pltpu.make_async_copy(hidden_hbm, hid.at[replica], own_sem)
    routing_copy = pltpu.make_async_copy(routing_hbm, routing_ref, routing_sem)
    tokens_copy = pltpu.make_async_copy(tokens_hbm, tokens_ref, tokens_sem)
    grads_copy = pltpu.make_async_copy(grads_ref, grads_hbm, grads_sem)
    turned_copy = pltpu.make_async_copy(turned_ref, turned_hbm, turned_sem)

    def peer(apart):
        return lax.rem(chip + apart + peers, peers) * 2 + core

    def place(replica_at, device):
        return replica_at * n_expert + device

    def hid_copy(at, band):
        deep = hid.shape[1] // BANDS
        block = hid.at[at, pl.ds(band * deep, deep)]
        return pltpu.make_async_remote_copy(
            block, block, hid_send.at[band], hid_recv.at[band],
            device_id=(other, index), device_id_type=MESH,
        )

    def moved(source, at, part, send, recv, apart, to):
        return pltpu.make_async_remote_copy(
            source, parts.at[part, at], send.at[part, apart], recv.at[part, apart],
            device_id=to, device_id_type=MESH,
        )

    def passed(at, part, send, recv, apart, to):
        return moved(parts.at[part, at], at, part, send, recv, apart, to)

    barrier = pltpu.get_barrier_semaphore()

    def greet(apart, carry):
        pl.semaphore_signal(barrier, inc=1, device_id=(replica, peer(apart)), device_id_type=MESH)
        return carry

    lax.fori_loop(1, peers, greet, 0)
    pl.semaphore_signal(barrier, inc=1, device_id=(replica, sibling), device_id_type=MESH)
    pl.semaphore_signal(barrier, inc=1, device_id=(other, index), device_id_type=MESH)

    routing_copy.start()
    tokens_copy.start()
    own_copy.start()
    for at in range(2):
        for which in range(2):
            ring_copy(at, which).start(priority=1)
    for at in range(PIECES):
        for which in range(2):
            near_copy(at, which).start(priority=1)

    routing_copy.wait()
    tokens_copy.wait()
    picks = placement(routing_ref[...], EXPERTS * 2 * CAP, CAP_BITS + 1)
    for part in range(2):
        at = part * half
        sent = jnp.dot(
            picks[0], tokens_ref[:, at : at + half], preferred_element_type=jnp.float32
        ) + jnp.dot(
            picks[1], tokens_ref[:, mine + at : mine + at + half], preferred_element_type=jnp.float32
        )
        out[part] = sent.astype(jnp.bfloat16).reshape(EXPERTS, 2 * CAP, half)
        parts[part, place(replica, index)] = out[part, index // shards]

    pl.semaphore_wait(barrier, peers + 1)

    own_at = place(replica, index)
    for part in range(2):
        def dispatch(apart, carry):
            to = peer(apart)
            moved(
                out.at[part, to // shards], own_at, part, row_send, row_recv, apart, (replica, to)
            ).start()
            return carry

        lax.fori_loop(1, peers, dispatch, 0)
    for part in range(2):
        own_block = out.at[part, index // shards]
        moved(own_block, own_at, part, far_send, far_recv, 0, (other, index)).start()
        moved(own_block, own_at, part, side_send, side_recv, 0, (replica, sibling)).start()

    own_copy.wait()
    for band in range(EARLY_BANDS):
        hid_copy(replica, band).start()

    def pass_on(part):
        def step(apart, carry):
            at = place(replica, peer(-apart))
            passed(at, part, row_send, row_recv, apart, (replica, sibling)).wait_recv()
            passed(at, part, far_send, far_recv, apart, (other, index)).start()
            passed(at, part, side_send, side_recv, apart, (replica, sibling)).start()
            return carry

        lax.fori_loop(1, peers, step, 0)

    def share(part):
        def step(apart, carry):
            at = place(other, peer(-apart))
            passed(at, part, far_send, far_recv, apart, (other, index)).wait_recv()
            passed(at, part, last_send, last_recv, apart, (replica, sibling)).start()
            return carry

        lax.fori_loop(0, peers, step, 0)

    def settle(part):
        def step(apart, carry):
            their = lax.rem(chip - apart + peers, peers) * 2 + 1 - core
            passed(
                place(replica, their), part, side_send, side_recv, apart, (replica, sibling)
            ).wait_recv()
            passed(
                place(other, their), part, last_send, last_recv, apart, (replica, sibling)
            ).wait_recv()
            return carry

        lax.fori_loop(0, peers, step, 0)
        for side, h in ((0, replica), (1, other)):
            pick = row_picker(group, h)
            for at in range(0, count, group):
                got = parts[part, pl.ds(at // CAP, group // CAP)].reshape(2 * group, half)
                rows[side, at : at + group, part * half : (part + 1) * half] = jnp.dot(
                    pick, got, preferred_element_type=jnp.float32
                ).astype(jnp.bfloat16)

    group = min(count, 128)

    def ring_part(at, which, column):
        return jnp.dot(
            rows[1, :, at * piece : (at + 1) * piece],
            ring[at % 2, which, :, column : column + tile],
            preferred_element_type=jnp.float32,
        )

    pass_on(0)
    pass_on(1)
    for band in range(EARLY_BANDS, BANDS):
        hid_copy(replica, band).start()
    share(0)
    settle(0)
    for which in range(2):
        ring_copy(0, which).wait()
    for column in range(0, span, tile):
        for which in range(2):
            pre[which, :, column : column + tile] = ring_part(0, which, column)
    for which in range(2):
        ring_copy(2, which).start(priority=1)
    share(1)
    for which in range(2):
        ring_copy(1, which).wait()
    for column in range(0, span, tile):
        for which in range(2):
            pre[which, :, column : column + tile] += ring_part(1, which, column)
    for which in range(2):
        ring_copy(3, which).start(priority=1)
    settle(1)
    for at in range(PIECES):
        for which in range(2):
            near_copy(at, which).wait()
    for column in range(0, span, tile):
        for which in range(2):
            pre[which, :, column : column + tile] += jnp.dot(
                rows[0], near[which, :, column : column + tile], preferred_element_type=jnp.float32
            )
    turned_ref[...] = rows[0].T
    turned_copy.start()
    for at in range(2, PIECES):
        for which in range(2):
            ring_copy(at, which).wait()
    for band in range(BANDS):
        hid_copy(other, band).wait_recv()
    for column in range(0, span, tile):
        gate_pre, up_pre = (
            pre[which, :, column : column + tile]
            + ring_part(2, which, column)
            + ring_part(3, which, column)
            for which in range(2)
        )
        grad_h = hid[:, :, column : column + tile].reshape(count, tile).astype(jnp.float32)
        sig = jax.nn.sigmoid(gate_pre)
        grads_ref[0, :, column : column + tile] = (
            grad_h * up_pre * sig * (1.0 + gate_pre * (1.0 - sig))
        ).astype(jnp.bfloat16)
        grads_ref[1, :, column : column + tile] = (grad_h * gate_pre * sig).astype(jnp.bfloat16)

    grads_copy.start()
    for at in range(0, mine, WIDE):
        back = lax.dot_general(
            grads_ref[0], near[0, at : at + WIDE], TRANSPOSED, preferred_element_type=jnp.float32
        ) + lax.dot_general(
            grads_ref[1], near[1, at : at + WIDE], TRANSPOSED, preferred_element_type=jnp.float32
        )
        kept[:, at : at + WIDE] = back.astype(jnp.bfloat16)

    for at in range(0, count, group):
        spread = jnp.dot(
            row_spreader(group, 0), kept[at : at + group, :half], preferred_element_type=jnp.float32
        ) + jnp.dot(
            row_spreader(group, 1), kept[at : at + group, half:], preferred_element_type=jnp.float32
        )
        part_ref[pl.ds(at // CAP, group // CAP)] = spread.astype(jnp.bfloat16).reshape(
            group // CAP, 2 * CAP, half
        )

    for band in range(BANDS):
        hid_copy(replica, band).wait_send()
    grads_copy.wait()
    turned_copy.wait()
    for part in range(2):
        def finish(apart, carry):
            passed(own_at, part, row_send, row_recv, apart, (replica, sibling)).wait_send()
            return carry

        def finish_moved(apart, carry):
            at = place(replica, peer(-apart))
            passed(at, part, side_send, side_recv, apart, (replica, sibling)).wait_send()
            passed(at, part, far_send, far_recv, apart, (other, index)).wait_send()
            passed(at, part, last_send, last_recv, apart, (replica, sibling)).wait_send()
            return carry

        lax.fori_loop(1, peers, finish, 0)
        lax.fori_loop(0, peers, finish_moved, 0)


def hidden_pass(routing, tokens, hidden, gate_weight, up_weight):
    n_dp, n_expert = lax.axis_size("dp"), lax.axis_size("expert")
    width = tokens.shape[1]
    span = gate_weight.shape[1]
    own_rows = hidden.shape[0]
    count = n_dp * own_rows
    peers = n_expert // 2
    mine = width // n_dp
    half = mine // 2
    vmem = pl.BlockSpec(memory_space=pltpu.VMEM)
    anywhere = pl.BlockSpec(memory_space=pl.ANY)
    blocks = n_dp * n_expert
    dma = pltpu.SemaphoreType.DMA
    per_peer = dma((2, peers))
    return pl.pallas_call(
        functools.partial(hidden_kernel, (n_dp, n_expert)),
        in_specs=[anywhere] * 5,
        out_specs=[anywhere, anywhere, vmem],
        out_shape=[
            jax.ShapeDtypeStruct((2, count, span), jnp.bfloat16),
            jax.ShapeDtypeStruct((mine, count), jnp.bfloat16),
            jax.ShapeDtypeStruct((blocks, 2 * CAP, half), jnp.bfloat16),
        ],
        scratch_shapes=[
            pltpu.VMEM(routing.shape, routing.dtype),
            pltpu.VMEM(tokens.shape, tokens.dtype),
            pltpu.VMEM((2, count, span), jnp.bfloat16),
            pltpu.VMEM((mine, count), jnp.bfloat16),
            pltpu.VMEM((2, EXPERTS, 2 * CAP, half), jnp.bfloat16),
            pltpu.VMEM((2, blocks, 2 * CAP, half), jnp.bfloat16),
            pltpu.VMEM((2, count, mine), jnp.bfloat16),
            pltpu.VMEM((n_dp, own_rows, span), jnp.bfloat16),
            pltpu.VMEM((2, mine, span), jnp.bfloat16),
            pltpu.VMEM((2, 2, mine // PIECES, span), jnp.bfloat16),
            pltpu.VMEM((2, count, span), jnp.float32),
            pltpu.VMEM((count, mine), jnp.bfloat16),
            dma((PIECES, 2)), dma((PIECES, 2)), dma(()), dma(()), dma(()), dma(()), dma(()),
            dma((BANDS,)), dma((BANDS,)),
            per_peer, per_peer, per_peer, per_peer,
            per_peer, per_peer, per_peer, per_peer,
        ],
        cost_estimate=pl.CostEstimate(
            flops=6 * count * width * span,
            bytes_accessed=4 * width * span,
            transcendentals=count * span,
        ),
        compiler_params=pltpu.CompilerParams(
            collective_id=0, has_side_effects=True, vmem_limit_bytes=KERNEL_MIB * MIB
        ),
    )(routing, tokens, hidden, gate_weight, up_weight)


def weight_kernel(turned_ref, grads_ref, gate_ref, up_ref):
    for at, out_ref in ((0, gate_ref), (1, up_ref)):
        out_ref[...] = jnp.dot(
            turned_ref[...], grads_ref[at], preferred_element_type=jnp.float32
        ).astype(out_ref.dtype)


def weight_pass(turned, grads):
    mine, count = turned.shape
    span = grads.shape[2]
    block = min(ROW_BLOCK, mine)
    result = jax.ShapeDtypeStruct((mine, span), jnp.bfloat16)
    out = pl.BlockSpec((block, span), lambda j: (j, 0))
    return pl.pallas_call(
        weight_kernel,
        grid=(mine // block,),
        in_specs=[
            pl.BlockSpec((block, count), lambda j: (j, 0)),
            pl.BlockSpec((2, count, span), lambda j: (0, 0, 0)),
        ],
        out_specs=[out, out],
        out_shape=[result, result],
        cost_estimate=pl.CostEstimate(
            flops=4 * count * mine * span, bytes_accessed=4 * mine * span, transcendentals=0
        ),
        compiler_params=pltpu.CompilerParams(
            dimension_semantics=("arbitrary",), vmem_limit_bytes=KERNEL_MIB * MIB
        ),
    )(turned, grads)


def return_kernel(shards, n_dp, routing_ref, back_ref, out_ref):
    blocks, deep, quarter = back_ref.shape
    sources = blocks // n_dp
    picks = placement(routing_ref[...], sources * deep, (deep * shards).bit_length() - 1)
    for replica in range(n_dp):
        got = back_ref[pl.ds(replica * sources, sources)].reshape(sources * deep, quarter)
        for h in range(2):
            at = (2 * replica + h) * quarter
            out_ref[:, at : at + quarter] = lax.dot_general(
                picks[h], got, LEADING, preferred_element_type=jnp.float32
            ).astype(out_ref.dtype)


def return_pass(routing, back, width):
    n_dp = lax.axis_size("dp")
    shards = lax.axis_size("expert") // EXPERTS
    vmem = pl.BlockSpec(memory_space=pltpu.VMEM)
    return pl.pallas_call(
        functools.partial(return_kernel, shards, n_dp),
        in_specs=[vmem, vmem],
        out_specs=vmem,
        out_shape=jax.ShapeDtypeStruct((routing.shape[1], width), jnp.bfloat16),
        compiler_params=pltpu.CompilerParams(vmem_limit_bytes=16 * MIB),
    )(routing, back)


def per_device(tokens, routing, hidden_grad, gate_weight, up_weight):
    routing = routing.T
    grads, turned, part = hidden_pass(routing, tokens, hidden_grad, gate_weight, up_weight)
    back = lax.all_to_all(part, ("dp", "expert"), split_axis=0, concat_axis=0, tiled=True)
    gate_weight_grad, up_weight_grad = weight_pass(turned, grads)
    token_grad = return_pass(routing, back, tokens.shape[1])
    return token_grad, gate_weight_grad, up_weight_grad


def solution(mesh):
    in_specs = (
        P(("dp", "expert"), None),
        P(("dp", "expert"), None),
        P(("dp", "expert"), None),
        P(None, "expert"),
        P(None, "expert"),
    )
    out_specs = (P(("dp", "expert"), None), P("dp", "expert"), P("dp", "expert"))
    return jax.shard_map(
        per_device, mesh=mesh, in_specs=in_specs, out_specs=out_specs, check_vma=False
    )
```

```python
import functools

import jax
import jax.numpy as jnp
from jax import lax
from jax.experimental import pallas as pl
from jax.experimental.pallas import tpu as pltpu
from jax.sharding import PartitionSpec as P


EXPERTS = 8
CAP = 4
CAP_BITS = CAP.bit_length() - 1
MIB = 1024 * 1024
KERNEL_MIB = 63

TILE = 512
WIDE = 512
GROUPS = 2
BANDS = 4
EARLY_BANDS = 1
ROW_BLOCK = 256
MESH = pl.DeviceIdType.MESH
TRANSPOSED = (((1,), (1,)), ((), ()))
LEADING = (((0,), (0,)), ((), ()))


def placement(routing, rows, expert_bits):
    count = routing.shape[1]
    row = lax.broadcasted_iota(jnp.int32, (rows, count), 0)
    expert, part = row >> expert_bits, (row >> CAP_BITS) & 1
    slot = (row & (CAP - 1)).astype(jnp.float32)
    first = jnp.where(routing[0:1] == expert, 1.0, 0.0)
    second = jnp.where(routing[1:2] == expert, 1.0, 0.0)
    earlier = jnp.where(
        lax.broadcasted_iota(jnp.int32, (count, count), 0)
        < lax.broadcasted_iota(jnp.int32, (count, count), 1),
        1.0,
        0.0,
    )
    before = jnp.dot(first + second, earlier, preferred_element_type=jnp.float32)
    placed = jnp.where(before == slot, first, 0.0) + jnp.where(before + first == slot, second, 0.0)
    return [jnp.where(part == h, placed, 0.0).astype(jnp.bfloat16) for h in range(2)]


def row_picker(rows, half):
    at = lax.broadcasted_iota(jnp.int32, (rows, 2 * rows), 0)
    column = lax.broadcasted_iota(jnp.int32, (rows, 2 * rows), 1)
    wanted = ((at >> CAP_BITS) << (CAP_BITS + 1)) + (at & (CAP - 1)) + half * CAP
    return jnp.where(column == wanted, 1.0, 0.0).astype(jnp.bfloat16)


def row_spreader(rows, half):
    column = lax.broadcasted_iota(jnp.int32, (2 * rows, rows), 1)
    at = lax.broadcasted_iota(jnp.int32, (2 * rows, rows), 0)
    wanted = ((column >> CAP_BITS) << (CAP_BITS + 1)) + (column & (CAP - 1)) + half * CAP
    return jnp.where(at == wanted, 1.0, 0.0).astype(jnp.bfloat16)


def hidden_kernel(
    dims,
    routing_hbm, tokens_hbm, hidden_hbm, gate_hbm, up_hbm,
    grads_hbm, turned_hbm, part_ref,
    routing_ref, tokens_ref, grads_ref, turned_ref, out, parts, rows, hid, near, ring, pre, total, kept,
    near_sem, ring_sem, own_sem, grads_sem, turned_sem, routing_sem, tokens_sem,
    hid_send, hid_recv, row_send, row_recv, side_send, side_recv,
    far_send, far_recv, last_send, last_recv,
):
    _, n_expert = dims
    replica, index = lax.axis_index("dp"), lax.axis_index("expert")
    shards = n_expert // EXPERTS
    peers = n_expert // 2
    chip, core = index // 2, index % 2
    sibling = chip * 2 + 1 - core
    other = 1 - replica
    _, count, mine = rows.shape
    half = parts.shape[3]
    span = gate_hbm.shape[1]
    wide = span // GROUPS
    tile = min(TILE, wide)
    weights = (gate_hbm, up_hbm)

    def near_copy(group, part, which):
        source = pl.ds(pl.multiple_of(replica * mine + part * half, half), half)
        columns = pl.ds(group * wide, wide)
        return pltpu.make_async_copy(
            weights[which].at[source, columns],
            near.at[which, pl.ds(part * half, half), columns],
            near_sem.at[group, part, which],
        )

    def ring_copy(group, part, which):
        source = pl.ds(pl.multiple_of(other * mine + part * half, half), half)
        return pltpu.make_async_copy(
            weights[which].at[source, pl.ds(group * wide, wide)],
            ring.at[part, which],
            ring_sem.at[group, part, which],
        )

    def loaded(group, part):
        for which in range(2):
            ring_copy(group, part, which).wait()
            near_copy(group, part, which).wait()

    def refill(part):
        for which in range(2):
            ring_copy(1, part, which).start(priority=1)

    own_copy = pltpu.make_async_copy(hidden_hbm, hid.at[replica], own_sem)
    routing_copy = pltpu.make_async_copy(routing_hbm, routing_ref, routing_sem)
    tokens_copy = pltpu.make_async_copy(tokens_hbm, tokens_ref, tokens_sem)
    grads_copy = pltpu.make_async_copy(grads_ref, grads_hbm, grads_sem)
    turned_copy = pltpu.make_async_copy(turned_ref, turned_hbm, turned_sem)

    def peer(apart):
        return lax.rem(chip + apart + peers, peers) * 2 + core

    def place(replica_at, device):
        return replica_at * n_expert + device

    def hid_copy(at, band):
        strip = span // BANDS
        block = hid.at[at, :, pl.ds(band * strip, strip)]
        return pltpu.make_async_remote_copy(
            block, block, hid_send.at[band], hid_recv.at[band],
            device_id=(other, index), device_id_type=MESH,
        )

    def moved(source, at, part, send, recv, apart, to):
        return pltpu.make_async_remote_copy(
            source, parts.at[part, at], send.at[part, apart], recv.at[part, apart],
            device_id=to, device_id_type=MESH,
        )

    def passed(at, part, send, recv, apart, to):
        return moved(parts.at[part, at], at, part, send, recv, apart, to)

    barrier = pltpu.get_barrier_semaphore()

    def greet(apart, carry):
        pl.semaphore_signal(barrier, inc=1, device_id=(replica, peer(apart)), device_id_type=MESH)
        return carry

    lax.fori_loop(1, peers, greet, 0)
    pl.semaphore_signal(barrier, inc=1, device_id=(replica, sibling), device_id_type=MESH)
    pl.semaphore_signal(barrier, inc=1, device_id=(other, index), device_id_type=MESH)

    routing_copy.start()
    tokens_copy.start()
    own_copy.start()
    for part in range(2):
        for which in range(2):
            ring_copy(0, part, which).start(priority=1)
            near_copy(0, part, which).start(priority=1)
    for part in range(2):
        for which in range(2):
            near_copy(1, part, which).start(priority=1)

    routing_copy.wait()
    tokens_copy.wait()
    picks = placement(routing_ref[...], EXPERTS * 2 * CAP, CAP_BITS + 1)
    for part in range(2):
        at = part * half
        sent = jnp.dot(
            picks[0], tokens_ref[:, at : at + half], preferred_element_type=jnp.float32
        ) + jnp.dot(
            picks[1], tokens_ref[:, mine + at : mine + at + half], preferred_element_type=jnp.float32
        )
        out[part] = sent.astype(jnp.bfloat16).reshape(EXPERTS, 2 * CAP, half)
        parts[part, place(replica, index)] = out[part, index // shards]

    pl.semaphore_wait(barrier, peers + 1)

    own_at = place(replica, index)
    for part in range(2):
        def dispatch(apart, carry):
            to = peer(apart)
            moved(
                out.at[part, to // shards], own_at, part, row_send, row_recv, apart, (replica, to)
            ).start()
            return carry

        lax.fori_loop(1, peers, dispatch, 0)
    for part in range(2):
        own_block = out.at[part, index // shards]
        moved(own_block, own_at, part, far_send, far_recv, 0, (other, index)).start()
        moved(own_block, own_at, part, side_send, side_recv, 0, (replica, sibling)).start()

    own_copy.wait()
    for band in range(EARLY_BANDS):
        hid_copy(replica, band).start()

    def pass_on(part):
        def step(apart, carry):
            at = place(replica, peer(-apart))
            passed(at, part, row_send, row_recv, apart, (replica, sibling)).wait_recv()
            passed(at, part, far_send, far_recv, apart, (other, index)).start()
            passed(at, part, side_send, side_recv, apart, (replica, sibling)).start()
            return carry

        lax.fori_loop(1, peers, step, 0)

    def share(part):
        def step(apart, carry):
            at = place(other, peer(-apart))
            passed(at, part, far_send, far_recv, apart, (other, index)).wait_recv()
            passed(at, part, last_send, last_recv, apart, (replica, sibling)).start()
            return carry

        lax.fori_loop(0, peers, step, 0)

    def settle(part):
        def step(apart, carry):
            their = lax.rem(chip - apart + peers, peers) * 2 + 1 - core
            passed(
                place(replica, their), part, side_send, side_recv, apart, (replica, sibling)
            ).wait_recv()
            passed(
                place(other, their), part, last_send, last_recv, apart, (replica, sibling)
            ).wait_recv()
            return carry

        lax.fori_loop(0, peers, step, 0)
        for side, h in ((0, replica), (1, other)):
            pick = row_picker(group, h)
            for at in range(0, count, group):
                got = parts[part, pl.ds(at // CAP, group // CAP)].reshape(2 * group, half)
                rows[side, at : at + group, part * half : (part + 1) * half] = jnp.dot(
                    pick, got, preferred_element_type=jnp.float32
                ).astype(jnp.bfloat16)

    group = min(count, 128)

    def product(part, which, column, start):
        features = slice(part * half, (part + 1) * half)
        return jnp.dot(
            rows[0, :, features],
            near[which, features, column : column + tile],
            preferred_element_type=jnp.float32,
        ) + jnp.dot(
            rows[1, :, features],
            ring[part, which, :, column - start : column - start + tile],
            preferred_element_type=jnp.float32,
        )

    def gradients(column, gate_pre, up_pre):
        grad_h = hid[:, :, column : column + tile].reshape(count, tile).astype(jnp.float32)
        sig = jax.nn.sigmoid(gate_pre)
        grads_ref[0, :, column : column + tile] = (
            grad_h * up_pre * sig * (1.0 + gate_pre * (1.0 - sig))
        ).astype(jnp.bfloat16)
        grads_ref[1, :, column : column + tile] = (grad_h * gate_pre * sig).astype(jnp.bfloat16)

    def arrived(bands):
        for band in bands:
            hid_copy(other, band).wait_recv()

    def back(at, columns):
        return lax.dot_general(
            grads_ref[0, :, columns], near[0, at : at + WIDE, columns], TRANSPOSED,
            preferred_element_type=jnp.float32,
        ) + lax.dot_general(
            grads_ref[1, :, columns], near[1, at : at + WIDE, columns], TRANSPOSED,
            preferred_element_type=jnp.float32,
        )

    pass_on(0)
    pass_on(1)
    for band in range(EARLY_BANDS, BANDS):
        hid_copy(replica, band).start()
    share(0)
    settle(0)
    loaded(0, 0)
    for column in range(0, wide, tile):
        for which in range(2):
            pre[which, :, column : column + tile] = product(0, which, column, 0)
    refill(0)
    share(1)
    settle(1)
    loaded(0, 1)
    arrived(range(BANDS // 2))
    for column in range(0, wide, tile):
        gate_pre, up_pre = (
            pre[which, :, column : column + tile] + product(1, which, column, 0) for which in range(2)
        )
        gradients(column, gate_pre, up_pre)
    refill(1)
    turned_ref[...] = rows[0].T
    turned_copy.start()
    columns = slice(0, wide)
    for at in range(0, mine, WIDE):
        total[:, at : at + WIDE] = back(at, columns)
    loaded(1, 0)
    loaded(1, 1)
    arrived(range(BANDS // 2, BANDS))
    for column in range(wide, span, tile):
        gate_pre, up_pre = (
            product(0, which, column, wide) + product(1, which, column, wide) for which in range(2)
        )
        gradients(column, gate_pre, up_pre)
    grads_copy.start()
    columns = slice(wide, span)
    for at in range(0, mine, WIDE):
        kept[:, at : at + WIDE] = (total[:, at : at + WIDE] + back(at, columns)).astype(jnp.bfloat16)

    for at in range(0, count, group):
        spread = jnp.dot(
            row_spreader(group, 0), kept[at : at + group, :half], preferred_element_type=jnp.float32
        ) + jnp.dot(
            row_spreader(group, 1), kept[at : at + group, half:], preferred_element_type=jnp.float32
        )
        part_ref[pl.ds(at // CAP, group // CAP)] = spread.astype(jnp.bfloat16).reshape(
            group // CAP, 2 * CAP, half
        )

    for band in range(BANDS):
        hid_copy(replica, band).wait_send()
    grads_copy.wait()
    turned_copy.wait()
    for part in range(2):
        def finish(apart, carry):
            passed(own_at, part, row_send, row_recv, apart, (replica, sibling)).wait_send()
            return carry

        def finish_moved(apart, carry):
            at = place(replica, peer(-apart))
            passed(at, part, side_send, side_recv, apart, (replica, sibling)).wait_send()
            passed(at, part, far_send, far_recv, apart, (other, index)).wait_send()
            passed(at, part, last_send, last_recv, apart, (replica, sibling)).wait_send()
            return carry

        lax.fori_loop(1, peers, finish, 0)
        lax.fori_loop(0, peers, finish_moved, 0)


def hidden_pass(routing, tokens, hidden, gate_weight, up_weight):
    n_dp, n_expert = lax.axis_size("dp"), lax.axis_size("expert")
    width = tokens.shape[1]
    span = gate_weight.shape[1]
    own_rows = hidden.shape[0]
    count = n_dp * own_rows
    peers = n_expert // 2
    mine = width // n_dp
    half = mine // 2
    vmem = pl.BlockSpec(memory_space=pltpu.VMEM)
    anywhere = pl.BlockSpec(memory_space=pl.ANY)
    blocks = n_dp * n_expert
    dma = pltpu.SemaphoreType.DMA
    per_peer = dma((2, peers))
    return pl.pallas_call(
        functools.partial(hidden_kernel, (n_dp, n_expert)),
        in_specs=[anywhere] * 5,
        out_specs=[anywhere, anywhere, vmem],
        out_shape=[
            jax.ShapeDtypeStruct((2, count, span), jnp.bfloat16),
            jax.ShapeDtypeStruct((mine, count), jnp.bfloat16),
            jax.ShapeDtypeStruct((blocks, 2 * CAP, half), jnp.bfloat16),
        ],
        scratch_shapes=[
            pltpu.VMEM(routing.shape, routing.dtype),
            pltpu.VMEM(tokens.shape, tokens.dtype),
            pltpu.VMEM((2, count, span), jnp.bfloat16),
            pltpu.VMEM((mine, count), jnp.bfloat16),
            pltpu.VMEM((2, EXPERTS, 2 * CAP, half), jnp.bfloat16),
            pltpu.VMEM((2, blocks, 2 * CAP, half), jnp.bfloat16),
            pltpu.VMEM((2, count, mine), jnp.bfloat16),
            pltpu.VMEM((n_dp, own_rows, span), jnp.bfloat16),
            pltpu.VMEM((2, mine, span), jnp.bfloat16),
            pltpu.VMEM((2, 2, half, span // GROUPS), jnp.bfloat16),
            pltpu.VMEM((2, count, span // GROUPS), jnp.float32),
            pltpu.VMEM((count, mine), jnp.float32),
            pltpu.VMEM((count, mine), jnp.bfloat16),
            dma((GROUPS, 2, 2)), dma((GROUPS, 2, 2)), dma(()), dma(()), dma(()), dma(()), dma(()),
            dma((BANDS,)), dma((BANDS,)),
            per_peer, per_peer, per_peer, per_peer,
            per_peer, per_peer, per_peer, per_peer,
        ],
        cost_estimate=pl.CostEstimate(
            flops=6 * count * width * span,
            bytes_accessed=4 * width * span,
            transcendentals=count * span,
        ),
        compiler_params=pltpu.CompilerParams(
            collective_id=0, has_side_effects=True, vmem_limit_bytes=KERNEL_MIB * MIB
        ),
    )(routing, tokens, hidden, gate_weight, up_weight)


def weight_kernel(turned_ref, grads_ref, gate_ref, up_ref):
    for at, out_ref in ((0, gate_ref), (1, up_ref)):
        out_ref[...] = jnp.dot(
            turned_ref[...], grads_ref[at], preferred_element_type=jnp.float32
        ).astype(out_ref.dtype)


def weight_pass(turned, grads):
    mine, count = turned.shape
    span = grads.shape[2]
    block = min(ROW_BLOCK, mine)
    result = jax.ShapeDtypeStruct((mine, span), jnp.bfloat16)
    out = pl.BlockSpec((block, span), lambda j: (j, 0))
    return pl.pallas_call(
        weight_kernel,
        grid=(mine // block,),
        in_specs=[
            pl.BlockSpec((block, count), lambda j: (j, 0)),
            pl.BlockSpec((2, count, span), lambda j: (0, 0, 0)),
        ],
        out_specs=[out, out],
        out_shape=[result, result],
        cost_estimate=pl.CostEstimate(
            flops=4 * count * mine * span, bytes_accessed=4 * mine * span, transcendentals=0
        ),
        compiler_params=pltpu.CompilerParams(
            dimension_semantics=("arbitrary",), vmem_limit_bytes=KERNEL_MIB * MIB
        ),
    )(turned, grads)


def return_kernel(shards, n_dp, routing_ref, back_ref, out_ref):
    blocks, deep, quarter = back_ref.shape
    sources = blocks // n_dp
    picks = placement(routing_ref[...], sources * deep, (deep * shards).bit_length() - 1)
    for replica in range(n_dp):
        got = back_ref[pl.ds(replica * sources, sources)].reshape(sources * deep, quarter)
        for h in range(2):
            at = (2 * replica + h) * quarter
            out_ref[:, at : at + quarter] = lax.dot_general(
                picks[h], got, LEADING, preferred_element_type=jnp.float32
            ).astype(out_ref.dtype)


def return_pass(routing, back, width):
    n_dp = lax.axis_size("dp")
    shards = lax.axis_size("expert") // EXPERTS
    vmem = pl.BlockSpec(memory_space=pltpu.VMEM)
    return pl.pallas_call(
        functools.partial(return_kernel, shards, n_dp),
        in_specs=[vmem, vmem],
        out_specs=vmem,
        out_shape=jax.ShapeDtypeStruct((routing.shape[1], width), jnp.bfloat16),
        compiler_params=pltpu.CompilerParams(vmem_limit_bytes=16 * MIB),
    )(routing, back)


def per_device(tokens, routing, hidden_grad, gate_weight, up_weight):
    routing = routing.T
    grads, turned, part = hidden_pass(routing, tokens, hidden_grad, gate_weight, up_weight)
    back = lax.all_to_all(part, ("dp", "expert"), split_axis=0, concat_axis=0, tiled=True)
    gate_weight_grad, up_weight_grad = weight_pass(turned, grads)
    token_grad = return_pass(routing, back, tokens.shape[1])
    return token_grad, gate_weight_grad, up_weight_grad


def solution(mesh):
    in_specs = (
        P(("dp", "expert"), None),
        P(("dp", "expert"), None),
        P(("dp", "expert"), None),
        P(None, "expert"),
        P(None, "expert"),
    )
    out_specs = (P(("dp", "expert"), None), P("dp", "expert"), P("dp", "expert"))
    return jax.shard_map(
        per_device, mesh=mesh, in_specs=in_specs, out_specs=out_specs, check_vma=False
    )
```
